32 devices in a mesh: gx: 4 (over z), gy: 8 (over y, x, core).
Axes of the slice: x: 2, y: 2, z: 4, core: 2. Of those that a mesh axis runs over, the one named last changes fastest.
Arguments:
- rhs: float32 [4, 8, 1, 3, 200, 128], P('gx', 'gy'), may hold values from -25 to 25
- stiff_inverse: bfloat16 [4, 8, 1, 1200, 1200], P('gx', 'gy'), may hold values from -2 to 6, as said below
- schur: bfloat16 [4, 8, 1, 1200, 1200], P('gx', 'gy'), may hold values from -2 to 6, as said below
- phi: bfloat16 [4, 8, 1, 24, 1200], P('gx', 'gy'), may hold values from -0.1875 to 0.1875
- coarse_inverse: float32 [192, 192], P(('gx', 'gy')), may hold values from -2 to 6, as said below
- incidence: int32 [4, 8, 1, 8], P('gx', 'gy'), may hold values from 0 to 63, as said below
- pairing: int32 [4, 8, 1, 3, 200], P('gx', 'gy'), may hold values from 0 to 199, as said below
Outputs:
- multipliers: float32 [4, 8, 1, 3, 200, 128], P('gx', 'gy')
- reduction: float32 [128], replicated
The draws below stay inside these ranges and needn't reach their ends.
Inputs may be any that keep to these rules, and one draw needn't show every extreme that they name: `stiff_inverse`: each block is symmetric positive definite. `schur`: each block is symmetric positive definite. `coarse_inverse`: symmetric positive definite. `incidence`: the corners of the subdomain grid, periodic in the first two dimensions, under an arbitrary numbering of the 64 nodes: corner c of subdomain (x, y, z) is the grid point (x + c % 2, y + (c // 2) % 2, z + c // 4), and subdomains that share a grid point name the same node. `pairing`: each row over the last dimension is a permutation of 0 to 199.
All inputs are finite; a program needn't handle non-finite values.
Results may differ from the reference program's by a relative error of at most 0.0027.
Values sent between devices are 32-bit elements; how exact they have to be, the bound alone decides.
A program may use at most 64 MiB of HBM per device.

```python
import math
import jax
import jax.numpy as jnp
from jax import lax

ORDER = 1200
FACE = 200
CORNER = 24
LOADS = 128
SUB_DEV = 1
ITERS = 2
GRID_X = 4
GRID_Y = 8
NODES = 64
COARSE = 192


def definite_block(key, size):
    noise = jax.random.normal(jax.random.fold_in(key, 1), (size, size), jnp.float32)
    coupled = (noise + noise.T) * (0.35 / math.sqrt(2.0 * size))
    diagonal = jax.random.uniform(jax.random.fold_in(key, 2), (size,), jnp.float32, 1.0, 2.0)
    block = coupled + jnp.diag(diagonal)
    return block


def block_stack(key):
    count = GRID_X * GRID_Y * SUB_DEV
    blocks = lax.map(lambda index: definite_block(jax.random.fold_in(key, index), ORDER).astype(jnp.bfloat16), jnp.arange(count))
    return blocks.reshape(GRID_X, GRID_Y, SUB_DEV, ORDER, ORDER)


def draw_stiff_inverse(key, part):
    return block_stack(jax.random.fold_in(key, 11))


def draw_schur(key, part):
    return block_stack(jax.random.fold_in(key, 23))


def draw_coarse_inverse(key, part):
    return definite_block(jax.random.fold_in(key, 37), COARSE)


def draw_rhs(key, part):
    count = GRID_X * GRID_Y * SUB_DEV
    shape = (GRID_X, GRID_Y, SUB_DEV, 3, FACE, LOADS)
    ramp = (jnp.arange(count, dtype=jnp.float32) / max(count - 1, 1)).reshape(GRID_X, GRID_Y, SUB_DEV, 1, 1, 1)
    scale = jnp.exp(math.log(3.0) * ramp)
    base = jax.random.truncated_normal(jax.random.fold_in(key, 63), -4.0, 4.0, shape, jnp.float32)
    return base * scale


def draw_incidence(key, part):
    dof_numbering = jax.random.permutation(jax.random.fold_in(key, 41), NODES).astype(jnp.int32)
    corner = jnp.arange(8, dtype=jnp.int32)
    first = jnp.arange(GRID_X, dtype=jnp.int32)[:, None, None, None] + corner % 2
    second = jnp.arange(GRID_Y, dtype=jnp.int32)[None, :, None, None] + corner // 2 % 2
    third = jnp.arange(SUB_DEV, dtype=jnp.int32)[None, None, :, None] + corner // 4
    node = (first % GRID_X * GRID_Y + second % GRID_Y) * (SUB_DEV + 1) + third
    return dof_numbering[node].astype(jnp.int32)


def draw_pairing(key, part):
    count = GRID_X * GRID_Y * SUB_DEV * 3
    subkeys = jax.random.split(jax.random.fold_in(key, 53), count)
    orderings = jax.vmap(lambda subkey: jax.random.permutation(subkey, FACE))(subkeys).astype(jnp.int32)
    return orderings.reshape(GRID_X, GRID_Y, SUB_DEV, 3, FACE)


def shard_levels(key, extent, pieces, low, high):
    def one(dim, blocks):
        draws = jax.random.uniform(jax.random.fold_in(jax.random.fold_in(key, 6), dim), (blocks,), jnp.float32, low / len(pieces), high / len(pieces))
        return jnp.repeat(jnp.exp(draws), extent[dim] // blocks).reshape((-1,) + (1,) * (len(extent) - dim - 1))

    loudness = one(*pieces[0])
    for cut in pieces[1:]:
        loudness = loudness * one(*cut)
    return loudness


def bell_draw(stream_key, dims, width, limit, pieces=(), held_as=jnp.bfloat16):
    values = jax.random.normal(stream_key, dims, jnp.float32) * width
    if len(pieces) > 0:
        values = shard_levels(stream_key, dims, pieces, -0.22, 0.18) * values
    return jnp.clip(values, min=-limit, max=limit).astype(held_as)


def setup_inputs(seed: int = 0) -> dict:
    key_list = jax.random.split(jax.random.key(seed), 8)
    rhs = draw_rhs(jax.random.fold_in(key_list[7], 71), 0)
    stiff_inverse = draw_stiff_inverse(jax.random.fold_in(key_list[7], 71), 0)
    schur = draw_schur(jax.random.fold_in(key_list[7], 71), 0)
    phi = bell_draw(key_list[3], (GRID_X, GRID_Y, SUB_DEV, CORNER, ORDER), ORDER ** -0.5, 0.1875, ((0, 4), (1, 8)))
    coarse_inverse = draw_coarse_inverse(jax.random.fold_in(key_list[7], 71), 0)
    incidence = draw_incidence(jax.random.fold_in(key_list[7], 71), 0)
    pairing = draw_pairing(jax.random.fold_in(key_list[7], 71), 0)
    return dict(rhs=rhs, stiff_inverse=stiff_inverse, schur=schur, phi=phi, coarse_inverse=coarse_inverse, incidence=incidence, pairing=pairing)


def reference(rhs, stiff_inverse, schur, phi, coarse_inverse, incidence, pairing):
    largest_index = lax.Precision.HIGHEST
    level = jnp.arange(SUB_DEV)[:, None]
    axis_id = jnp.arange(3)[None, :]
    active = jnp.where((level == SUB_DEV - 1) & (axis_id == 2), 0.0, 1.0)
    active = active.astype(jnp.float32)[None, None, :, :, None, None]
    inverse_pairing = jnp.argsort(pairing, axis=-1).astype(jnp.int32)
    coupling_matrix = phi.astype(jnp.float32)
    flat_ids = incidence.reshape(-1).astype(jnp.int32)

    def transpose_jump(values):
        masked = values * active
        moved = jnp.take_along_axis(masked, inverse_pairing[..., None], axis=4)
        lower_x = jnp.roll(moved[:, :, :, 0], 1, axis=0)
        lower_y = jnp.roll(moved[:, :, :, 1], 1, axis=1)
        lower_z = jnp.concatenate([jnp.zeros_like(moved[:, :, :1, 2]), moved[:, :, :-1, 2]], axis=2)
        return jnp.stack([-lower_x, masked[:, :, :, 0], -lower_y, masked[:, :, :, 1], -lower_z, masked[:, :, :, 2]], axis=3)

    def jump_field(field):
        upper_x = jnp.roll(field[:, :, :, 0], -1, axis=0)
        upper_y = jnp.roll(field[:, :, :, 2], -1, axis=1)
        upper_z = jnp.concatenate([field[:, :, 1:, 4], jnp.zeros_like(field[:, :, :1, 4])], axis=2)
        neighbour = jnp.stack([upper_x, upper_y, upper_z], axis=3)
        paired = jnp.take_along_axis(neighbour, pairing[..., None], axis=4)
        higher = jnp.stack([field[:, :, :, 1], field[:, :, :, 3], field[:, :, :, 5]], axis=3)
        return (higher - paired) * active

    def apply_local(matrices, field):
        flat_matrices = matrices.reshape(-1, ORDER, ORDER)
        flat_field = field.reshape(-1, ORDER, LOADS).astype(jnp.bfloat16)
        result = lax.map(lambda both: jnp.dot(both[0], both[1], preferred_element_type=jnp.float32), (flat_matrices, flat_field))
        return result.reshape(GRID_X, GRID_Y, SUB_DEV, 6, FACE, LOADS)

    def operator(values):
        field = transpose_jump(values)
        corner_load = jnp.einsum('xyzco,xyzor->xyzcr', coupling_matrix, field.reshape(GRID_X, GRID_Y, SUB_DEV, ORDER, LOADS), precision=largest_index)
        coarse_load = jax.ops.segment_sum(corner_load.reshape(-1, 3, LOADS), flat_ids, num_segments=NODES).reshape(COARSE, LOADS)
        coarse_solution = jnp.dot(coarse_inverse, coarse_load, precision=largest_index)
        corner_values = coarse_solution.reshape(NODES, 3, LOADS)[flat_ids].reshape(GRID_X, GRID_Y, SUB_DEV, CORNER, LOADS)
        spread_operator = jnp.einsum('xyzco,xyzcr->xyzor', coupling_matrix, corner_values, precision=largest_index)
        displacement = apply_local(stiff_inverse, field) + spread_operator.reshape(GRID_X, GRID_Y, SUB_DEV, 6, FACE, LOADS)
        return jump_field(displacement)

    def precondition(values):
        field = 0.5 * transpose_jump(values)
        return 0.5 * jump_field(apply_local(schur, field))

    def inner_product(left, right):
        return jnp.sum(left * right, axis=(0, 1, 2, 3, 4))

    residual = rhs * active
    multipliers = jnp.zeros_like(residual)
    preconditioned = precondition(residual)
    energy = inner_product(residual, preconditioned)
    start_energy = energy
    direction = preconditioned
    for iteration in range(ITERS):
        product_field = operator(direction)
        alpha = energy / inner_product(direction, product_field)
        multipliers = multipliers + alpha * direction
        residual = residual - alpha * product_field
        preconditioned = precondition(residual)
        energy_next = inner_product(residual, preconditioned)
        if iteration + 1 < ITERS:
            direction = preconditioned + (energy_next / energy) * direction
        energy = energy_next
    return multipliers, energy / start_energy
```

```python
import functools

import jax
import jax.numpy as jnp
from jax import lax
from jax.experimental import pallas as pl
from jax.experimental.pallas import tpu as pltpu
from jax.sharding import PartitionSpec as P

ITERS = 2
EXCHANGES = 2 * ITERS
SUMS = 2 * ITERS + 1
GROUP = 32
MESH = pl.DeviceIdType.MESH
F32 = jnp.float32
BF16 = jnp.bfloat16


def split(value, parts):
    pieces = []
    for _ in range(parts):
        piece = value.astype(BF16)
        pieces.append(piece)
        value = value - piece.astype(F32)
    return pieces


def narrow_dot(matrix, value, parts):
    width = value.shape[1]
    product = jnp.dot(
        matrix, jnp.concatenate(split(value, parts), axis=1), preferred_element_type=F32
    )
    total = product[:, (parts - 1) * width :]
    for part in range(parts - 2, -1, -1):
        total = total + product[:, part * width : (part + 1) * width]
    return total


def full_dot(left, right):
    return jnp.dot(left, right, precision=lax.Precision.HIGHEST, preferred_element_type=F32)


def window(face, faces):
    start = face * faces // 128 * 128
    offset = face * faces - start
    return start, offset, -(-(offset + faces) // 128) * 128


def square_window(face, faces):
    start = face * faces // 128 * 128
    offset = face * faces - start
    return start, offset, -(-(offset + faces) // 256) * 256


def kernel(
    nx, ny, rhs_hbm, stiff_hbm, schur_hbm, phi_ref, cinv_ref, inc_ref, pair_ref,
    mult_ref, reduction_ref,
    rhs_v, stiff, schur, phi_f, phi_p, phi_t, near_t, near_phi, got_rhs, got_pair, got,
    field, way, image, sums_out, sums_in, ids_out, ids_in, cinv_in, cinv, chosen, assemble,
    load_out, load_in,
    local_sem, setup_send, setup_recv, face_send, face_recv, sum_send, sum_recv,
    all_send, all_recv, load_send, load_recv,
):
    n = nx * ny
    faces = rhs_v.shape[1]
    interface = stiff.shape[0]
    coarse = cinv.shape[0]
    ix, iy = lax.axis_index("gx"), lax.axis_index("gy")
    me = ix * ny + iy
    up_x, down_x = lax.rem(ix + 1, nx), lax.rem(ix + nx - 1, nx)
    up_y, down_y = lax.rem(iy + 1, ny), lax.rem(iy + ny - 1, ny)
    across = [(down_x, iy), (up_x, iy), (ix, down_y), (ix, up_y)]
    rows = [pl.ds(f * faces, faces) for f in range(6)]

    loads = [
        pltpu.make_async_copy(rhs_hbm, rhs_v, local_sem.at[0]),
        pltpu.make_async_copy(schur_hbm, schur, local_sem.at[1]),
        pltpu.make_async_copy(stiff_hbm, stiff, local_sem.at[2]),
    ]
    for copy in loads:
        copy.start()

    def peer(step):
        other = lax.rem(me + step, n)
        return (lax.div(other, ny), lax.rem(other, ny))

    barrier = pltpu.get_barrier_semaphore()

    def greet(step, carry):
        pl.semaphore_signal(barrier, inc=1, device_id=peer(step), device_id_type=MESH)
        return carry

    lax.fori_loop(1, n, greet, 0)

    corners = phi_f.shape[0]
    row = lax.broadcasted_iota(jnp.int32, (corners, corners), 0)
    col = lax.broadcasted_iota(jnp.int32, (corners, corners), 1)
    nodes = corners // 3
    order = jnp.where(col == 3 * lax.rem(row, nodes) + lax.div(row, nodes), 1.0, 0.0)
    phi_f[...] = jnp.dot(order.astype(BF16), phi_ref[...], preferred_element_type=F32)
    ids = jnp.broadcast_to(inc_ref[...].astype(F32), (nodes, nodes))
    diag = lax.broadcasted_iota(jnp.int32, (nodes, nodes), 0) == lax.broadcasted_iota(
        jnp.int32, (nodes, nodes), 1
    )
    ids = jnp.sum(jnp.where(diag, ids, 0.0), axis=1, keepdims=True)
    ids = jnp.broadcast_to(ids, ids_out.shape)
    ids_out[...] = ids
    ids_in[me] = ids
    cinv_in[me] = cinv_ref[...]

    loads[0].wait()
    pl.semaphore_wait(barrier, n - 1)

    def send(src, dst, send_sem, recv_sem, target):
        copy = pltpu.make_async_remote_copy(
            src_ref=src, dst_ref=dst, send_sem=send_sem, recv_sem=recv_sem,
            device_id=target, device_id_type=MESH,
        )
        copy.start()
        return copy

    def to_all(src, slots, send_sem, recv_sem):
        def step(k, carry):
            send(src, slots.at[me], send_sem, recv_sem, peer(k))
            return carry

        lax.fori_loop(1, n, step, 0)

    def wait_all(slots, sem):
        whole = slots.at[pl.ds(0, n - 1)]
        pltpu.make_async_copy(whole, whole, sem).wait()

    setup = []
    for a in range(2):
        setup.append(send(pair_ref, got_pair.at[a], setup_send.at[a], setup_recv.at[a],
                          across[2 * a + 1]))
    for a in range(2):
        setup.append(send(rhs_v.at[a], got_rhs.at[a], setup_send.at[2 + a],
                          setup_recv.at[2 + a], across[2 * a + 1]))
    for f in range(4):
        start, _, width = window(f, faces)
        partner = f ^ 1
        setup.append(send(phi_f.at[:, pl.ds(start, width)],
                          near_phi.at[partner, :, pl.ds(0, width)],
                          setup_send.at[4 + f], setup_recv.at[4 + partner], across[f]))
    to_all(ids_out, ids_in, all_send.at[0], all_recv.at[0])
    to_all(cinv_ref, cinv_in, all_send.at[1], all_recv.at[1])

    def turned(pair_row, offset, width):
        lanes = lax.broadcasted_iota(jnp.int32, (1, width), 1)
        if width > faces:
            pair_row = jnp.concatenate(
                [pair_row, jnp.zeros((1, width - faces), jnp.int32)], axis=1
            )
        if offset:
            pair_row = pltpu.roll(pair_row, offset, axis=1)
        inside = (lanes >= offset) & (lanes < offset + faces)
        target = jnp.where(inside, pair_row + offset, lanes)
        place = lax.broadcasted_iota(jnp.int32, (width, width), 0)
        return jnp.where(place == target, 1.0, 0.0)

    turns = []
    for a in range(2):
        setup[a].wait_recv()
        start, offset, width = square_window(2 * a, faces)
        by_col = turned(got_pair[a, a : a + 1, :], offset, width)
        turns.append((start, width, by_col.T.astype(BF16), by_col.astype(BF16)))

    def reorder(matrix):
        for start, width, by_row, _ in turns:
            band = matrix[pl.ds(start, width), :]
            matrix[pl.ds(start, width), :] = jnp.dot(
                by_row, band, preferred_element_type=F32
            ).astype(BF16)
        for start, width, _, by_col in turns:
            band = matrix[:, pl.ds(start, width)]
            matrix[:, pl.ds(start, width)] = jnp.dot(
                band, by_col, preferred_element_type=F32
            ).astype(BF16)

    loads[1].wait()
    reorder(schur)

    def apply_local(matrix, low, k):
        sent = []
        for half in range(3):
            part = pl.ds(2 * half * faces, 2 * faces)
            image[k, part, :] = jnp.dot(matrix[part, :], low, preferred_element_type=F32)
            if half < 2:
                for f in (2 * half, 2 * half + 1):
                    sent.append(send(image.at[k, rows[f]], got.at[k, f ^ 1],
                                     face_send.at[k, f], face_recv.at[k, f ^ 1], across[f]))
        return sent

    def start_sum(partial, k):
        total = jnp.sum(partial, axis=0, keepdims=True)
        sums_out[k] = total
        sums_in[k, me] = total
        to_all(sums_out.at[k], sums_in.at[k], sum_send.at[k], sum_recv.at[k])

    def finish_sum(k):
        wait_all(sums_in.at[k], sum_recv.at[k])
        return jnp.sum(sums_in[k], axis=0)

    def wait_faces(k):
        for f in range(4):
            pltpu.make_async_copy(got.at[k, f], got.at[k, f], face_recv.at[k, f]).wait()

    zeros = jnp.zeros((2 * faces, field.shape[1]), F32)
    for a in range(2):
        setup[2 + a].wait_recv()
        field[rows[2 * a], :] = -got_rhs[a]
        field[rows[2 * a + 1], :] = rhs_v[a]
    field[pl.ds(4 * faces, 2 * faces), :] = zeros
    for k in range(ITERS):
        way[k, pl.ds(4 * faces, 2 * faces), :] = zeros

    sent = []

    def precondition(k, s):
        half = 0.5 * field[...]
        sent.extend(apply_local(schur, half.astype(BF16), k))
        start_sum(half * image[k], s)

    precondition(0, 0)

    loads[2].wait()
    reorder(stiff)
    phi_p[...] = phi_f[...].astype(BF16)
    for start, width, _, by_col in turns:
        phi_p[:, pl.ds(start, width)] = jnp.dot(
            phi_p[:, pl.ds(start, width)], by_col, preferred_element_type=F32
        ).astype(BF16)
    phi_t[...] = phi_p[...].astype(F32).T.astype(BF16)

    def dof_rows(block):
        return jnp.concatenate([3.0 * block + i for i in range(3)], axis=block.ndim - 2)

    group = min(GROUP, n)

    def placed(g):
        block = dof_rows(ids_in[pl.ds(g * group, group)])
        line = block.reshape(group * corners, 128).T[0:1]
        spot = lax.broadcasted_iota(jnp.int32, (coarse, group * corners), 0).astype(F32)
        return jnp.where(spot == line, 1.0, 0.0).astype(BF16)

    def prepare_coarse():
        for f in range(4):
            _, offset, width = window(f ^ 1, faces)
            setup[4 + (f ^ 1)].wait_recv()
            tall = near_phi[f, :, pl.ds(0, width)].T[offset : offset + faces]
            if f % 2:
                by_row = turned(pair_ref[f // 2 : f // 2 + 1, :], 0, faces).T
                tall = jnp.dot(by_row.astype(BF16), tall.astype(BF16),
                               preferred_element_type=F32)
            near_t[f] = tall.astype(BF16)
        wait_all(ids_in, all_recv.at[0])
        if n == group:
            assemble[...] = placed(0)
        wait_all(cinv_in, all_recv.at[1])
        block_rows = cinv_in.shape[1]

        def pack(g, carry):
            block = jnp.concatenate([cinv_in[4 * g + i] for i in range(4)], axis=0)
            cinv[pl.ds(pl.multiple_of(4 * block_rows * g, 8), 4 * block_rows), :] = block
            return carry

        lax.fori_loop(0, n // 4, pack, 0)
        picks = []
        for gx, gy in across + [(ix, iy)]:
            dofs = dof_rows(ids_in[gx * ny + gy])[:, 0:1]
            spot = lax.broadcasted_iota(jnp.int32, (corners, coarse), 1).astype(F32)
            picks.append(jnp.where(spot == dofs, 1.0, 0.0))
        pick = jnp.concatenate(picks, axis=0).astype(BF16)
        chosen[...] = narrow_dot(pick, cinv[...], 3)

    energy = start_energy = previous = None
    alphas = []
    for it in range(ITERS):
        k = 2 * it
        wait_faces(k)
        if it:
            following = finish_sum(2 * it)
            ratio = following / energy
            energy = following
        for f in range(4):
            moved = 0.5 * (image[k, rows[f], :] - got[k, f])
            if it:
                moved = moved + ratio * way[it - 1, rows[f], :]
            way[it, rows[f], :] = moved
        walk = way[it]
        corner_load = narrow_dot(phi_p[...], walk, 2)
        load_out[it] = corner_load
        load_in[it, me] = corner_load
        to_all(load_out.at[it], load_in.at[it], load_send.at[it], load_recv.at[it])
        sent.extend(apply_local(stiff, walk.astype(BF16), k + 1))
        start_sum(walk * image[k + 1], 2 * it + 1)
        if it == 0:
            prepare_coarse()
            energy = start_energy = finish_sum(0)
        wait_all(load_in.at[it], load_recv.at[it])

        def gather(g, total):
            if n > group:
                assemble[...] = placed(g)
            block = load_in[it, pl.ds(g * group, group)].reshape(group * corners, -1)
            return total + narrow_dot(assemble[...], block, 3)

        coarse_load = lax.fori_loop(
            0, n // group, gather, jnp.zeros((coarse, field.shape[1]), F32)
        )
        solution_rows = full_dot(cinv[...], coarse_load)
        near = full_dot(chosen[...], coarse_load)
        coarse_part = jnp.sum(coarse_load * solution_rows, axis=0, keepdims=True)
        own = narrow_dot(phi_t[...], near[4 * corners :], 2)
        wait_faces(k + 1)
        alpha = energy / (finish_sum(2 * it + 1) + coarse_part)
        alphas.append(alpha)
        for f in range(4):
            other = narrow_dot(near_t[f], near[f * corners : (f + 1) * corners], 2)
            jump = (image[k + 1, rows[f], :] - got[k + 1, f]) + (
                own[f * faces : (f + 1) * faces] - other
            )
            field[rows[f], :] = field[rows[f], :] - alpha * jump
        if it + 1 < ITERS:
            precondition(k + 2, 2 * it + 2)
        else:
            half = 0.5 * field[...]
            product = jnp.dot(schur[...], half.astype(BF16), preferred_element_type=F32)
            start_sum(half * product, 2 * it + 2)

    for a in range(2):
        total = alphas[0] * way[0, rows[2 * a + 1], :]
        for it in range(1, ITERS):
            total = total + alphas[it] * way[it, rows[2 * a + 1], :]
        mult_ref[a] = total
    mult_ref[2] = jnp.zeros(mult_ref.shape[1:], F32)

    for copy in setup + sent:
        copy.wait_send()
    wait_all(ids_in, all_send.at[0])
    wait_all(cinv_in, all_send.at[1])
    for it in range(ITERS):
        wait_all(load_in.at[it], load_send.at[it])
    reduction_ref[...] = finish_sum(SUMS - 1) / start_energy
    for k in range(SUMS):
        wait_all(sums_in.at[k], sum_send.at[k])


def local(nx, ny, rhs, stiff_inverse, schur, phi, coarse_inverse, incidence, pairing):
    n = nx * ny
    faces, cases = rhs.shape[4], rhs.shape[5]
    interface = stiff_inverse.shape[3]
    corners = phi.shape[3]
    coarse_rows, coarse = coarse_inverse.shape
    nodes = incidence.shape[3]
    group = min(GROUP, n)
    wide = max(window(f, faces)[2] for f in range(4))
    vmem = pl.BlockSpec(memory_space=pltpu.VMEM)
    anywhere = pl.BlockSpec(memory_space=pl.ANY)
    dma = pltpu.SemaphoreType.DMA
    multipliers, reduction = pl.pallas_call(
        functools.partial(kernel, nx, ny),
        out_shape=(
            jax.ShapeDtypeStruct((3, faces, cases), F32),
            jax.ShapeDtypeStruct((1, cases), F32),
        ),
        in_specs=[anywhere] * 3 + [vmem] * 4,
        out_specs=(vmem, vmem),
        scratch_shapes=[
            pltpu.VMEM((3, faces, cases), F32),
            pltpu.VMEM((interface, interface), BF16),
            pltpu.VMEM((interface, interface), BF16),
            pltpu.VMEM((corners, interface), F32),
            pltpu.VMEM((corners, interface), BF16),
            pltpu.VMEM((interface, corners), BF16),
            pltpu.VMEM((4, faces, corners), BF16),
            pltpu.VMEM((4, corners, wide), F32),
            pltpu.VMEM((2, faces, cases), F32),
            pltpu.VMEM((2, 3, faces), jnp.int32),
            pltpu.VMEM((EXCHANGES, 4, faces, cases), F32),
            pltpu.VMEM((interface, cases), F32),
            pltpu.VMEM((ITERS, interface, cases), F32),
            pltpu.VMEM((EXCHANGES, interface, cases), F32),
            pltpu.VMEM((SUMS, 1, cases), F32),
            pltpu.VMEM((SUMS, n, 1, cases), F32),
            pltpu.VMEM((nodes, 128), F32),
            pltpu.VMEM((n, nodes, 128), F32),
            pltpu.VMEM((n, coarse_rows, coarse), F32),
            pltpu.VMEM((coarse, coarse), F32),
            pltpu.VMEM((5 * corners, coarse), F32),
            pltpu.VMEM((coarse, group * corners), BF16),
            pltpu.VMEM((ITERS, corners, cases), F32),
            pltpu.VMEM((ITERS, n, corners, cases), F32),
            dma((3,)),
            dma((8,)),
            dma((8,)),
            dma((EXCHANGES, 4)),
            dma((EXCHANGES, 4)),
            dma((SUMS,)),
            dma((SUMS,)),
            dma((2,)),
            dma((2,)),
            dma((ITERS,)),
            dma((ITERS,)),
        ],
        compiler_params=pltpu.CompilerParams(
            collective_id=0, has_side_effects=True, vmem_limit_bytes=67043328
        ),
    )(
        rhs.reshape(3, faces, cases),
        stiff_inverse.reshape(interface, interface),
        schur.reshape(interface, interface),
        phi.reshape(corners, interface),
        coarse_inverse,
        incidence.reshape(1, nodes),
        pairing.reshape(3, faces),
    )
    return multipliers.reshape(rhs.shape), reduction.reshape(cases)


def solution(mesh):
    nx, ny = mesh.shape["gx"], mesh.shape["gy"]
    return jax.shard_map(
        functools.partial(local, nx, ny),
        mesh=mesh,
        in_specs=(
            P("gx", "gy", None, None, None, None),
            P("gx", "gy", None, None, None),
            P("gx", "gy", None, None, None),
            P("gx", "gy", None, None, None),
            P(("gx", "gy"), None),
            P("gx", "gy", None, None),
            P("gx", "gy", None, None, None),
        ),
        out_specs=(P("gx", "gy", None, None, None, None), P()),
        check_vma=False,
    )
```

```python
import functools

import jax
import jax.numpy as jnp
from jax import lax
from jax.experimental import pallas as pl
from jax.experimental.pallas import tpu as pltpu
from jax.sharding import PartitionSpec as P

ITERS = 2
EXCHANGES = 2 * ITERS
SUMS = 2 * ITERS + 1
GROUP = 8
MESH = pl.DeviceIdType.MESH
F32 = jnp.float32
BF16 = jnp.bfloat16


def split(value, parts):
    pieces = []
    for _ in range(parts):
        piece = value.astype(BF16)
        pieces.append(piece)
        value = value - piece.astype(F32)
    return pieces


def narrow_dot(matrix, value, parts):
    width = value.shape[1]
    product = jnp.dot(
        matrix, jnp.concatenate(split(value, parts), axis=1), preferred_element_type=F32
    )
    total = product[:, (parts - 1) * width :]
    for part in range(parts - 2, -1, -1):
        total = total + product[:, part * width : (part + 1) * width]
    return total


def full_dot(left, right):
    return jnp.dot(left, right, precision=lax.Precision.HIGHEST, preferred_element_type=F32)


def window(face, faces):
    start = face * faces // 128 * 128
    offset = face * faces - start
    return start, offset, -(-(offset + faces) // 128) * 128


def square_window(face, faces):
    start = face * faces // 128 * 128
    offset = face * faces - start
    return start, offset, -(-(offset + faces) // 256) * 256


def kernel(
    nx, ny, rhs_hbm, stiff_hbm, schur_hbm, phi_ref, cinv_ref, inc_ref, pair_ref,
    mult_ref, reduction_ref,
    rhs_v, stiff, schur, phi_f, phi_p, phi_t, near_t, near_phi, got_rhs, got_pair, got,
    field, way, image, sums_out, sums_in, ids_out, ids_in, cinv_in, cinv, chosen, assemble,
    load_x, load_y,
    local_sem, setup_send, setup_recv, face_send, face_recv, sum_send, sum_recv,
    all_send, all_recv, load_send, load_recv,
):
    n = nx * ny
    faces = rhs_v.shape[1]
    interface = stiff.shape[0]
    coarse = cinv.shape[0]
    ix, iy = lax.axis_index("gx"), lax.axis_index("gy")
    me = ix * ny + iy
    up_x, down_x = lax.rem(ix + 1, nx), lax.rem(ix + nx - 1, nx)
    up_y, down_y = lax.rem(iy + 1, ny), lax.rem(iy + ny - 1, ny)
    across = [(down_x, iy), (up_x, iy), (ix, down_y), (ix, up_y)]
    rows = [pl.ds(f * faces, faces) for f in range(6)]

    loads = [
        pltpu.make_async_copy(rhs_hbm, rhs_v, local_sem.at[0]),
        pltpu.make_async_copy(schur_hbm, schur, local_sem.at[1]),
        pltpu.make_async_copy(stiff_hbm, stiff, local_sem.at[2]),
    ]
    for copy in loads:
        copy.start()

    ways_x = [ix] + [lax.rem(ix + d, nx) for d in range(1, nx)]
    ways_y = [iy] + [lax.rem(iy + d, ny) for d in range(1, ny)]
    peers_x = [(x, iy) for x in ways_x[1:]]
    peers_y = [(ix, y) for y in ways_y[1:]]

    def each_peer(act):
        if n <= 64:
            for x in range(nx):
                for y in range(ny):
                    if x or y:
                        act((ways_x[x], ways_y[y]))
            return

        def step(k, carry):
            other = lax.rem(me + k, n)
            act((lax.div(other, ny), lax.rem(other, ny)))
            return carry

        lax.fori_loop(1, n, step, 0)

    barrier = pltpu.get_barrier_semaphore()
    each_peer(lambda target: pl.semaphore_signal(
        barrier, inc=1, device_id=target, device_id_type=MESH))

    corners = phi_f.shape[0]
    row = lax.broadcasted_iota(jnp.int32, (corners, corners), 0)
    col = lax.broadcasted_iota(jnp.int32, (corners, corners), 1)
    nodes = corners // 3
    side, half_rows = nodes // 2, corners // 2
    inner = lax.rem(row, half_rows)
    corner = lax.div(row, half_rows) + 2 * lax.rem(inner, side)
    order = jnp.where(col == 3 * corner + lax.div(inner, side), 1.0, 0.0)
    phi_f[...] = jnp.dot(order.astype(BF16), phi_ref[...], preferred_element_type=F32)
    ids = jnp.broadcast_to(inc_ref[...].astype(F32), (nodes, nodes))
    row = lax.broadcasted_iota(jnp.int32, (nodes, nodes), 0)
    col = lax.broadcasted_iota(jnp.int32, (nodes, nodes), 1)
    diag = col == lax.div(row, side) + 2 * lax.rem(row, side)
    ids = jnp.sum(jnp.where(diag, ids, 0.0), axis=1, keepdims=True)
    ids = jnp.broadcast_to(ids, ids_out.shape)
    ids_out[...] = ids
    ids_in[iy, ix] = ids
    cinv_in[iy, ix] = cinv_ref[...]

    loads[0].wait()
    pl.semaphore_wait(barrier, n - 1)

    def send(src, dst, send_sem, recv_sem, target):
        copy = pltpu.make_async_remote_copy(
            src_ref=src, dst_ref=dst, send_sem=send_sem, recv_sem=recv_sem,
            device_id=target, device_id_type=MESH,
        )
        copy.start()
        return copy

    def to_all(src, slots, send_sem, recv_sem):
        each_peer(lambda target: send(src, slots.at[me], send_sem, recv_sem, target))

    def to_line(src, dst, send_sem, recv_sem, targets):
        for target in targets:
            send(src, dst, send_sem, recv_sem, target)

    def wait_all(slots, sem):
        whole = slots.at[pl.ds(0, slots.shape[0] - 1)]
        pltpu.make_async_copy(whole, whole, sem).wait()

    setup = []
    for a in range(2):
        setup.append(send(pair_ref, got_pair.at[a], setup_send.at[a], setup_recv.at[a],
                          across[2 * a + 1]))
    for a in range(2):
        setup.append(send(rhs_v.at[a], got_rhs.at[a], setup_send.at[2 + a],
                          setup_recv.at[2 + a], across[2 * a + 1]))
    for f in range(4):
        start, _, width = window(f, faces)
        partner = f ^ 1
        setup.append(send(phi_f.at[:, pl.ds(start, width)],
                          near_phi.at[partner, :, pl.ds(0, width)],
                          setup_send.at[4 + f], setup_recv.at[4 + partner], across[f]))
    to_line(ids_out, ids_in.at[iy, ix], all_send.at[0], all_recv.at[0], peers_x)
    to_line(cinv_ref, cinv_in.at[iy, ix], all_send.at[1], all_recv.at[1], peers_x)

    def turned(pair_row, offset, width):
        lanes = lax.broadcasted_iota(jnp.int32, (1, width), 1)
        if width > faces:
            pair_row = jnp.concatenate(
                [pair_row, jnp.zeros((1, width - faces), jnp.int32)], axis=1
            )
        if offset:
            pair_row = pltpu.roll(pair_row, offset, axis=1)
        inside = (lanes >= offset) & (lanes < offset + faces)
        target = jnp.where(inside, pair_row + offset, lanes)
        place = lax.broadcasted_iota(jnp.int32, (width, width), 0)
        return jnp.where(place == target, 1.0, 0.0)

    turns = []
    for a in range(2):
        setup[a].wait_recv()
        start, offset, width = square_window(2 * a, faces)
        by_col = turned(got_pair[a, a : a + 1, :], offset, width)
        turns.append((start, width, by_col.T.astype(BF16), by_col.astype(BF16)))

    def reorder(matrix):
        for start, width, by_row, _ in turns:
            band = matrix[pl.ds(start, width), :]
            matrix[pl.ds(start, width), :] = jnp.dot(
                by_row, band, preferred_element_type=F32
            ).astype(BF16)
        for start, width, _, by_col in turns:
            band = matrix[:, pl.ds(start, width)]
            matrix[:, pl.ds(start, width)] = jnp.dot(
                band, by_col, preferred_element_type=F32
            ).astype(BF16)

    wait_all(ids_in.at[iy], all_recv.at[0])
    wait_all(cinv_in.at[iy], all_recv.at[1])
    to_line(ids_in.at[iy], ids_in.at[iy], all_send.at[2], all_recv.at[2], peers_y)
    to_line(cinv_in.at[iy], cinv_in.at[iy], all_send.at[3], all_recv.at[3], peers_y)
    loads[1].wait()
    reorder(schur)

    def apply_local(matrix, low, k):
        sent = []
        for half in range(3):
            part = pl.ds(2 * half * faces, 2 * faces)
            image[k, part, :] = jnp.dot(matrix[part, :], low, preferred_element_type=F32)
            if half < 2:
                for f in (2 * half, 2 * half + 1):
                    sent.append(send(image.at[k, rows[f]], got.at[k, f ^ 1],
                                     face_send.at[k, f], face_recv.at[k, f ^ 1], across[f]))
        return sent

    def start_sum(partial, k):
        total = jnp.sum(partial, axis=0, keepdims=True)
        sums_out[k] = total
        sums_in[k, me] = total
        to_all(sums_out.at[k], sums_in.at[k], sum_send.at[k], sum_recv.at[k])

    def finish_sum(k):
        wait_all(sums_in.at[k], sum_recv.at[k])
        return jnp.sum(sums_in[k], axis=0)

    def wait_faces(k):
        for f in range(4):
            pltpu.make_async_copy(got.at[k, f], got.at[k, f], face_recv.at[k, f]).wait()

    zeros = jnp.zeros((2 * faces, field.shape[1]), F32)
    for a in range(2):
        setup[2 + a].wait_recv()
        field[rows[2 * a], :] = -got_rhs[a]
        field[rows[2 * a + 1], :] = rhs_v[a]
    field[pl.ds(4 * faces, 2 * faces), :] = zeros
    for k in range(ITERS):
        way[k, pl.ds(4 * faces, 2 * faces), :] = zeros

    sent = []

    def precondition(k, s):
        half = 0.5 * field[...]
        sent.extend(apply_local(schur, half.astype(BF16), k))
        start_sum(half * image[k], s)

    precondition(0, 0)

    loads[2].wait()
    reorder(stiff)
    phi_p[...] = phi_f[...].astype(BF16)
    for start, width, _, by_col in turns:
        phi_p[:, pl.ds(start, width)] = jnp.dot(
            phi_p[:, pl.ds(start, width)], by_col, preferred_element_type=F32
        ).astype(BF16)
    phi_t[...] = phi_p[...].astype(F32).T.astype(BF16)

    group = min(GROUP, ny)
    width = nx * half_rows

    def dof_rows(block):
        return jnp.concatenate(
            [3.0 * block[h * side : (h + 1) * side] + i for h in range(2) for i in range(3)],
            axis=0,
        )

    def placed(g):
        block = ids_in[pl.ds(g * group, group)].reshape(group * nx // 2, 2, nodes, 128)
        block = jnp.concatenate(
            [3.0 * block[:, b, 0:side] + i for b in range(2) for i in range(3)], axis=1
        )
        line = block.reshape(group * width, 128).T[0:1]
        spot = lax.broadcasted_iota(jnp.int32, (coarse, group * width), 0).astype(F32)
        return jnp.where(spot == line, 1.0, 0.0).astype(BF16)

    def prepare_coarse():
        for f in range(4):
            _, offset, width = window(f ^ 1, faces)
            setup[4 + (f ^ 1)].wait_recv()
            tall = near_phi[f, :, pl.ds(0, width)].T[offset : offset + faces]
            if f % 2:
                by_row = turned(pair_ref[f // 2 : f // 2 + 1, :], 0, faces).T
                tall = jnp.dot(by_row.astype(BF16), tall.astype(BF16),
                               preferred_element_type=F32)
            near_t[f] = tall.astype(BF16)
        wait_all(ids_in, all_recv.at[2])
        if ny == group:
            assemble[...] = placed(0)
        wait_all(cinv_in, all_recv.at[3])
        block_rows = 4 * cinv_in.shape[2]
        for x in range(nx):
            def pack(g, carry):
                block = jnp.concatenate([cinv_in[4 * g + i, x] for i in range(4)], axis=0)
                place = (x * (ny // 4) + g) * block_rows
                cinv[pl.ds(pl.multiple_of(place, 8), block_rows), :] = block
                return carry

            lax.fori_loop(0, ny // 4, pack, 0, unroll=ny <= 8)
        picks = []
        for gx, gy in across + [(ix, iy)]:
            dofs = dof_rows(ids_in[gy, gx])[:, 0:1]
            spot = lax.broadcasted_iota(jnp.int32, (corners, coarse), 1).astype(F32)
            picks.append(jnp.where(spot == dofs, 1.0, 0.0))
        pick = jnp.concatenate(picks, axis=0).astype(BF16)
        chosen[...] = narrow_dot(pick, cinv[...], 3)

    energy = start_energy = previous = None
    alphas = []
    for it in range(ITERS):
        k = 2 * it
        wait_faces(k)
        if it:
            following = finish_sum(2 * it)
            ratio = following / energy
            energy = following
        for f in range(4):
            moved = 0.5 * (image[k, rows[f], :] - got[k, f])
            if it:
                moved = moved + ratio * way[it - 1, rows[f], :]
            way[it, rows[f], :] = moved
        walk = way[it]
        corner_load = narrow_dot(phi_p[...], walk, 2)
        load_x[it, ix] = corner_load
        to_line(load_x.at[it, ix], load_x.at[it, ix], load_send.at[it], load_recv.at[it],
                peers_x)
        sent.extend(apply_local(stiff, walk.astype(BF16), k + 1))
        start_sum(walk * image[k + 1], 2 * it + 1)
        wait_all(load_x.at[it], load_recv.at[it])
        for pair in range(nx // 2):
            joined = [
                load_x[it, x, 0:half_rows] + load_x[it, (x - 1) % nx, half_rows:corners]
                for x in (2 * pair, 2 * pair + 1)
            ]
            load_y[it, iy, pl.ds(pair * corners, corners)] = jnp.concatenate(joined, axis=0)
        to_line(load_y.at[it, iy], load_y.at[it, iy], load_send.at[ITERS + it],
                load_recv.at[ITERS + it], peers_y)
        if it == 0:
            prepare_coarse()
            energy = start_energy = finish_sum(0)
        wait_all(load_y.at[it], load_recv.at[ITERS + it])

        def gather(g, total):
            if ny > group:
                assemble[...] = placed(g)
            block = load_y[it, pl.ds(g * group, group)].reshape(group * width, -1)
            return total + narrow_dot(assemble[...], block, 3)

        coarse_load = lax.fori_loop(
            0, ny // group, gather, jnp.zeros((coarse, field.shape[1]), F32)
        )
        solution_rows = full_dot(cinv[...], coarse_load)
        near = full_dot(chosen[...], coarse_load)
        coarse_part = jnp.sum(coarse_load * solution_rows, axis=0, keepdims=True)
        own = narrow_dot(phi_t[...], near[4 * corners :], 2)
        wait_faces(k + 1)
        alpha = energy / (finish_sum(2 * it + 1) + coarse_part)
        alphas.append(alpha)
        for f in range(4):
            other = narrow_dot(near_t[f], near[f * corners : (f + 1) * corners], 2)
            jump = (image[k + 1, rows[f], :] - got[k + 1, f]) + (
                own[f * faces : (f + 1) * faces] - other
            )
            field[rows[f], :] = field[rows[f], :] - alpha * jump
        if it + 1 < ITERS:
            precondition(k + 2, 2 * it + 2)
        else:
            half = 0.5 * field[...]
            product = jnp.dot(schur[...], half.astype(BF16), preferred_element_type=F32)
            start_sum(half * product, 2 * it + 2)

    for a in range(2):
        total = alphas[0] * way[0, rows[2 * a + 1], :]
        for it in range(1, ITERS):
            total = total + alphas[it] * way[it, rows[2 * a + 1], :]
        mult_ref[a] = total
    mult_ref[2] = jnp.zeros(mult_ref.shape[1:], F32)

    for copy in setup + sent:
        copy.wait_send()
    wait_all(ids_in.at[iy], all_send.at[0])
    wait_all(cinv_in.at[iy], all_send.at[1])
    wait_all(ids_in, all_send.at[2])
    wait_all(cinv_in, all_send.at[3])
    for it in range(ITERS):
        wait_all(load_x.at[it], load_send.at[it])
        wait_all(load_y.at[it], load_send.at[ITERS + it])
    reduction_ref[...] = finish_sum(SUMS - 1) / start_energy
    for k in range(SUMS):
        wait_all(sums_in.at[k], sum_send.at[k])


def local(nx, ny, rhs, stiff_inverse, schur, phi, coarse_inverse, incidence, pairing):
    n = nx * ny
    faces, cases = rhs.shape[4], rhs.shape[5]
    interface = stiff_inverse.shape[3]
    corners = phi.shape[3]
    coarse_rows, coarse = coarse_inverse.shape
    nodes = incidence.shape[3]
    group = min(GROUP, ny)
    wide = max(window(f, faces)[2] for f in range(4))
    vmem = pl.BlockSpec(memory_space=pltpu.VMEM)
    anywhere = pl.BlockSpec(memory_space=pl.ANY)
    dma = pltpu.SemaphoreType.DMA
    multipliers, reduction = pl.pallas_call(
        functools.partial(kernel, nx, ny),
        out_shape=(
            jax.ShapeDtypeStruct((3, faces, cases), F32),
            jax.ShapeDtypeStruct((1, cases), F32),
        ),
        in_specs=[anywhere] * 3 + [vmem] * 4,
        out_specs=(vmem, vmem),
        scratch_shapes=[
            pltpu.VMEM((3, faces, cases), F32),
            pltpu.VMEM((interface, interface), BF16),
            pltpu.VMEM((interface, interface), BF16),
            pltpu.VMEM((corners, interface), F32),
            pltpu.VMEM((corners, interface), BF16),
            pltpu.VMEM((interface, corners), BF16),
            pltpu.VMEM((4, faces, corners), BF16),
            pltpu.VMEM((4, corners, wide), F32),
            pltpu.VMEM((2, faces, cases), F32),
            pltpu.VMEM((2, 3, faces), jnp.int32),
            pltpu.VMEM((EXCHANGES, 4, faces, cases), F32),
            pltpu.VMEM((interface, cases), F32),
            pltpu.VMEM((ITERS, interface, cases), F32),
            pltpu.VMEM((EXCHANGES, interface, cases), F32),
            pltpu.VMEM((SUMS, 1, cases), F32),
            pltpu.VMEM((SUMS, n, 1, cases), F32),
            pltpu.VMEM((nodes, 128), F32),
            pltpu.VMEM((ny, nx, nodes, 128), F32),
            pltpu.VMEM((ny, nx, coarse_rows, coarse), F32),
            pltpu.VMEM((coarse, coarse), F32),
            pltpu.VMEM((5 * corners, coarse), F32),
            pltpu.VMEM((coarse, group * nx * corners // 2), BF16),
            pltpu.VMEM((ITERS, nx, corners, cases), F32),
            pltpu.VMEM((ITERS, ny, nx * corners // 2, cases), F32),
            dma((3,)),
            dma((8,)),
            dma((8,)),
            dma((EXCHANGES, 4)),
            dma((EXCHANGES, 4)),
            dma((SUMS,)),
            dma((SUMS,)),
            dma((4,)),
            dma((4,)),
            dma((2 * ITERS,)),
            dma((2 * ITERS,)),
        ],
        compiler_params=pltpu.CompilerParams(
            collective_id=0, has_side_effects=True, vmem_limit_bytes=67043328
        ),
    )(
        rhs.reshape(3, faces, cases),
        stiff_inverse.reshape(interface, interface),
        schur.reshape(interface, interface),
        phi.reshape(corners, interface),
        coarse_inverse,
        incidence.reshape(1, nodes),
        pairing.reshape(3, faces),
    )
    return multipliers.reshape(rhs.shape), reduction.reshape(cases)


def solution(mesh):
    nx, ny = mesh.shape["gx"], mesh.shape["gy"]
    return jax.shard_map(
        functools.partial(local, nx, ny),
        mesh=mesh,
        in_specs=(
            P("gx", "gy", None, None, None, None),
            P("gx", "gy", None, None, None),
            P("gx", "gy", None, None, None),
            P("gx", "gy", None, None, None),
            P(("gx", "gy"), None),
            P("gx", "gy", None, None),
            P("gx", "gy", None, None, None),
        ),
        out_specs=(P("gx", "gy", None, None, None, None), P()),
        check_vma=False,
    )
```

```python
import functools

import jax
import jax.numpy as jnp
from jax import lax
from jax.experimental import pallas as pl
from jax.experimental.pallas import tpu as pltpu
from jax.sharding import PartitionSpec as P

ITERS = 2
EXCHANGES = 2 * ITERS
SUMS = 2 * ITERS + 1
GROUP = 8
MESH = pl.DeviceIdType.MESH
F32 = jnp.float32
BF16 = jnp.bfloat16


def split(value, parts):
    pieces = []
    for _ in range(parts):
        piece = value.astype(BF16)
        pieces.append(piece)
        value = value - piece.astype(F32)
    return pieces


def narrow_dot(matrix, value, parts):
    width = value.shape[1]
    product = jnp.dot(
        matrix, jnp.concatenate(split(value, parts), axis=1), preferred_element_type=F32
    )
    total = product[:, (parts - 1) * width :]
    for part in range(parts - 2, -1, -1):
        total = total + product[:, part * width : (part + 1) * width]
    return total


def full_dot(left, right):
    return jnp.dot(left, right, precision=lax.Precision.HIGHEST, preferred_element_type=F32)


def window(face, faces):
    start = face * faces // 128 * 128
    offset = face * faces - start
    return start, offset, -(-(offset + faces) // 128) * 128


def square_window(face, faces):
    start = face * faces // 128 * 128
    offset = face * faces - start
    return start, offset, -(-(offset + faces) // 256) * 256


def kernel(
    nx, ny, rhs_hbm, stiff_hbm, schur_hbm, phi_ref, cinv_ref, inc_ref, pair_ref,
    mult_ref, reduction_ref,
    rhs_v, stiff, schur, phi_f, phi_p, phi_t, near_t, near_phi, got_rhs, got_pair, got,
    field, way, image, sums_out, sums_in, ids_out, ids_in, cinv_in, cinv, chosen, assemble,
    load_x, load_y,
    local_sem, setup_send, setup_recv, face_send, face_recv, sum_send, sum_recv,
    all_send, all_recv, load_send, load_recv,
):
    n = nx * ny
    faces = rhs_v.shape[1]
    interface = stiff.shape[0]
    coarse = cinv.shape[0]
    ix, iy = lax.axis_index("gx"), lax.axis_index("gy")
    me = ix * ny + iy
    up_x, down_x = lax.rem(ix + 1, nx), lax.rem(ix + nx - 1, nx)
    up_y, down_y = lax.rem(iy + 1, ny), lax.rem(iy + ny - 1, ny)
    across = [(down_x, iy), (up_x, iy), (ix, down_y), (ix, up_y)]
    rows = [pl.ds(f * faces, faces) for f in range(6)]

    loads = [
        pltpu.make_async_copy(rhs_hbm, rhs_v, local_sem.at[0]),
        pltpu.make_async_copy(schur_hbm, schur, local_sem.at[1]),
        pltpu.make_async_copy(stiff_hbm, stiff, local_sem.at[2]),
    ]
    for copy in loads:
        copy.start()

    ways_x = [ix] + [lax.rem(ix + d, nx) for d in range(1, nx)]
    ways_y = [iy] + [lax.rem(iy + d, ny) for d in range(1, ny)]
    peers_x = [(x, iy) for x in ways_x[1:]]
    peers_y = [(ix, y) for y in ways_y[1:]]

    def each_peer(act):
        if n <= 64:
            for x in range(nx):
                for y in range(ny):
                    if x or y:
                        act((ways_x[x], ways_y[y]))
            return

        def step(k, carry):
            other = lax.rem(me + k, n)
            act((lax.div(other, ny), lax.rem(other, ny)))
            return carry

        lax.fori_loop(1, n, step, 0)

    barrier = pltpu.get_barrier_semaphore()
    each_peer(lambda target: pl.semaphore_signal(
        barrier, inc=1, device_id=target, device_id_type=MESH))

    corners = phi_f.shape[0]
    row = lax.broadcasted_iota(jnp.int32, (corners, corners), 0)
    col = lax.broadcasted_iota(jnp.int32, (corners, corners), 1)
    nodes = corners // 3
    side, half_rows = nodes // 2, corners // 2
    inner = lax.rem(row, half_rows)
    corner = lax.div(row, half_rows) + 2 * lax.rem(inner, side)
    order = jnp.where(col == 3 * corner + lax.div(inner, side), 1.0, 0.0)
    phi_f[...] = jnp.dot(order.astype(BF16), phi_ref[...], preferred_element_type=F32)
    ids = jnp.broadcast_to(inc_ref[...].astype(F32), (nodes, nodes))
    row = lax.broadcasted_iota(jnp.int32, (nodes, nodes), 0)
    col = lax.broadcasted_iota(jnp.int32, (nodes, nodes), 1)
    diag = col == lax.div(row, side) + 2 * lax.rem(row, side)
    ids = jnp.sum(jnp.where(diag, ids, 0.0), axis=1, keepdims=True)
    ids = jnp.broadcast_to(ids, ids_out.shape)
    ids_out[...] = ids
    ids_in[iy, ix] = ids
    cinv_in[iy, ix] = cinv_ref[...]

    loads[0].wait()
    pl.semaphore_wait(barrier, n - 1)

    def send(src, dst, send_sem, recv_sem, target):
        copy = pltpu.make_async_remote_copy(
            src_ref=src, dst_ref=dst, send_sem=send_sem, recv_sem=recv_sem,
            device_id=target, device_id_type=MESH,
        )
        copy.start()
        return copy

    def to_all(src, slots, send_sem, recv_sem):
        each_peer(lambda target: send(src, slots.at[me], send_sem, recv_sem, target))

    def to_line(src, dst, send_sem, recv_sem, targets):
        for target in targets:
            send(src, dst, send_sem, recv_sem, target)

    def wait_all(slots, sem):
        whole = slots.at[pl.ds(0, slots.shape[0] - 1)]
        pltpu.make_async_copy(whole, whole, sem).wait()

    setup = []
    for a in range(2):
        setup.append(send(pair_ref, got_pair.at[a], setup_send.at[a], setup_recv.at[a],
                          across[2 * a + 1]))
    for a in range(2):
        setup.append(send(rhs_v.at[a], got_rhs.at[a], setup_send.at[2 + a],
                          setup_recv.at[2 + a], across[2 * a + 1]))
    for f in range(4):
        start, _, width = window(f, faces)
        partner = f ^ 1
        setup.append(send(phi_f.at[:, pl.ds(start, width)],
                          near_phi.at[partner, :, pl.ds(0, width)],
                          setup_send.at[4 + f], setup_recv.at[4 + partner], across[f]))
    to_line(ids_out, ids_in.at[iy, ix], all_send.at[0], all_recv.at[0], peers_x)
    to_line(cinv_ref, cinv_in.at[iy, ix], all_send.at[1], all_recv.at[1], peers_x)

    def turned(pair_row, offset, width):
        lanes = lax.broadcasted_iota(jnp.int32, (1, width), 1)
        if width > faces:
            pair_row = jnp.concatenate(
                [pair_row, jnp.zeros((1, width - faces), jnp.int32)], axis=1
            )
        if offset:
            pair_row = pltpu.roll(pair_row, offset, axis=1)
        inside = (lanes >= offset) & (lanes < offset + faces)
        target = jnp.where(inside, pair_row + offset, lanes)
        place = lax.broadcasted_iota(jnp.int32, (width, width), 0)
        return jnp.where(place == target, 1.0, 0.0)

    turns = []
    for a in range(2):
        setup[a].wait_recv()
        start, offset, width = square_window(2 * a, faces)
        by_col = turned(got_pair[a, a : a + 1, :], offset, width)
        turns.append((start, width, by_col.T.astype(BF16), by_col.astype(BF16)))

    def reorder(matrix):
        for start, width, by_row, _ in turns:
            band = matrix[pl.ds(start, width), :]
            matrix[pl.ds(start, width), :] = jnp.dot(
                by_row, band, preferred_element_type=F32
            ).astype(BF16)
        for start, width, _, by_col in turns:
            band = matrix[:, pl.ds(start, width)]
            matrix[:, pl.ds(start, width)] = jnp.dot(
                band, by_col, preferred_element_type=F32
            ).astype(BF16)

    wait_all(ids_in.at[iy], all_recv.at[0])
    wait_all(cinv_in.at[iy], all_recv.at[1])
    to_line(ids_in.at[iy], ids_in.at[iy], all_send.at[2], all_recv.at[2], peers_y)
    to_line(cinv_in.at[iy], cinv_in.at[iy], all_send.at[3], all_recv.at[3], peers_y)
    loads[1].wait()
    reorder(schur)

    def apply_local(matrix, low, k):
        sent = []
        for half in range(3):
            part = pl.ds(2 * half * faces, 2 * faces)
            image[k, part, :] = jnp.dot(matrix[part, :], low, preferred_element_type=F32)
            if half < 2:
                for f in (2 * half, 2 * half + 1):
                    sent.append(send(image.at[k, rows[f]], got.at[k, f ^ 1],
                                     face_send.at[k, f], face_recv.at[k, f ^ 1], across[f]))
        return sent

    def start_sum(partial, k):
        total = jnp.sum(partial, axis=0, keepdims=True)
        sums_out[k] = total
        sums_in[k, me] = total
        to_all(sums_out.at[k], sums_in.at[k], sum_send.at[k], sum_recv.at[k])

    def finish_sum(k):
        wait_all(sums_in.at[k], sum_recv.at[k])
        return jnp.sum(sums_in[k], axis=0)

    def wait_faces(k):
        for f in range(4):
            pltpu.make_async_copy(got.at[k, f], got.at[k, f], face_recv.at[k, f]).wait()

    zeros = jnp.zeros((2 * faces, field.shape[1]), F32)
    for a in range(2):
        setup[2 + a].wait_recv()
        field[rows[2 * a], :] = -got_rhs[a]
        field[rows[2 * a + 1], :] = rhs_v[a]
    field[pl.ds(4 * faces, 2 * faces), :] = zeros
    for k in range(ITERS):
        way[k, pl.ds(4 * faces, 2 * faces), :] = zeros

    sent = []

    def precondition(k, s):
        half = 0.5 * field[...]
        sent.extend(apply_local(schur, half.astype(BF16), k))
        start_sum(half * image[k], s)

    precondition(0, 0)

    loads[2].wait()
    reorder(stiff)
    phi_p[...] = phi_f[...].astype(BF16)
    for start, width, _, by_col in turns:
        phi_p[:, pl.ds(start, width)] = jnp.dot(
            phi_p[:, pl.ds(start, width)], by_col, preferred_element_type=F32
        ).astype(BF16)
    phi_t[...] = phi_p[...].astype(F32).T.astype(BF16)

    group = min(GROUP, ny)
    width = nx * half_rows

    def dof_rows(block):
        return jnp.concatenate(
            [3.0 * block[h * side : (h + 1) * side] + i for h in range(2) for i in range(3)],
            axis=0,
        )

    def placed(g):
        block = ids_in[pl.ds(g * group, group)].reshape(group * nx // 2, 2, nodes, 128)
        block = jnp.concatenate(
            [3.0 * block[:, b, 0:side] + i for b in range(2) for i in range(3)], axis=1
        )
        line = block.reshape(group * width, 128).T[0:1]
        spot = lax.broadcasted_iota(jnp.int32, (coarse, group * width), 0).astype(F32)
        return jnp.where(spot == line, 1.0, 0.0).astype(BF16)

    def prepare_coarse():
        for f in range(4):
            _, offset, width = window(f ^ 1, faces)
            setup[4 + (f ^ 1)].wait_recv()
            tall = near_phi[f, :, pl.ds(0, width)].T[offset : offset + faces]
            if f % 2:
                by_row = turned(pair_ref[f // 2 : f // 2 + 1, :], 0, faces).T
                tall = jnp.dot(by_row.astype(BF16), tall.astype(BF16),
                               preferred_element_type=F32)
            near_t[f] = tall.astype(BF16)
        wait_all(ids_in, all_recv.at[2])
        if ny == group:
            assemble[...] = placed(0)
        wait_all(cinv_in, all_recv.at[3])
        block_rows = 4 * cinv_in.shape[2]
        for x in range(nx):
            def pack(g, carry):
                block = jnp.concatenate([cinv_in[4 * g + i, x] for i in range(4)], axis=0)
                place = (x * (ny // 4) + g) * block_rows
                cinv[pl.ds(pl.multiple_of(place, 8), block_rows), :] = block
                return carry

            lax.fori_loop(0, ny // 4, pack, 0, unroll=ny <= 8)
        picks = []
        for gx, gy in across + [(ix, iy)]:
            dofs = dof_rows(ids_in[gy, gx])[:, 0:1]
            spot = lax.broadcasted_iota(jnp.int32, (corners, coarse), 1).astype(F32)
            picks.append(jnp.where(spot == dofs, 1.0, 0.0))
        pick = jnp.concatenate(picks, axis=0).astype(BF16)
        chosen[...] = narrow_dot(pick, cinv[...], 3)

    energy = start_energy = previous = None
    alphas = []
    for it in range(ITERS):
        k = 2 * it
        wait_faces(k)
        if it:
            following = finish_sum(2 * it)
            ratio = following / energy
            energy = following
        for f in range(4):
            moved = 0.5 * (image[k, rows[f], :] - got[k, f])
            if it:
                moved = moved + ratio * way[it - 1, rows[f], :]
            way[it, rows[f], :] = moved
        walk = way[it]
        corner_load = narrow_dot(phi_p[...], walk, 2)
        load_x[it, ix] = corner_load
        to_line(load_x.at[it, ix], load_x.at[it, ix], load_send.at[it], load_recv.at[it],
                peers_x)
        sent.extend(apply_local(stiff, walk.astype(BF16), k + 1))
        wait_all(load_x.at[it], load_recv.at[it])
        for pair in range(nx // 2):
            joined = [
                load_x[it, x, 0:half_rows] + load_x[it, (x - 1) % nx, half_rows:corners]
                for x in (2 * pair, 2 * pair + 1)
            ]
            load_y[it, iy, pl.ds(pair * corners, corners)] = jnp.concatenate(joined, axis=0)
        to_line(load_y.at[it, iy], load_y.at[it, iy], load_send.at[ITERS + it],
                load_recv.at[ITERS + it], peers_y)
        start_sum(walk * image[k + 1], 2 * it + 1)
        if it == 0:
            prepare_coarse()
            energy = start_energy = finish_sum(0)
        wait_all(load_y.at[it], load_recv.at[ITERS + it])

        def gather(g, total):
            if ny > group:
                assemble[...] = placed(g)
            block = load_y[it, pl.ds(g * group, group)].reshape(group * width, -1)
            return total + narrow_dot(assemble[...], block, 3)

        coarse_load = lax.fori_loop(
            0, ny // group, gather, jnp.zeros((coarse, field.shape[1]), F32)
        )
        solution_rows = full_dot(cinv[...], coarse_load)
        near = full_dot(chosen[...], coarse_load)
        coarse_part = jnp.sum(coarse_load * solution_rows, axis=0, keepdims=True)
        own = narrow_dot(phi_t[...], near[4 * corners :], 2)
        wait_faces(k + 1)
        alpha = energy / (finish_sum(2 * it + 1) + coarse_part)
        alphas.append(alpha)
        for f in range(4):
            other = narrow_dot(near_t[f], near[f * corners : (f + 1) * corners], 2)
            jump = (image[k + 1, rows[f], :] - got[k + 1, f]) + (
                own[f * faces : (f + 1) * faces] - other
            )
            field[rows[f], :] = field[rows[f], :] - alpha * jump
        if it + 1 < ITERS:
            precondition(k + 2, 2 * it + 2)
        else:
            half = 0.5 * field[...]
            product = jnp.dot(schur[...], half.astype(BF16), preferred_element_type=F32)
            start_sum(half * product, 2 * it + 2)

    for a in range(2):
        total = alphas[0] * way[0, rows[2 * a + 1], :]
        for it in range(1, ITERS):
            total = total + alphas[it] * way[it, rows[2 * a + 1], :]
        mult_ref[a] = total
    mult_ref[2] = jnp.zeros(mult_ref.shape[1:], F32)

    for copy in setup + sent:
        copy.wait_send()
    wait_all(ids_in.at[iy], all_send.at[0])
    wait_all(cinv_in.at[iy], all_send.at[1])
    wait_all(ids_in, all_send.at[2])
    wait_all(cinv_in, all_send.at[3])
    for it in range(ITERS):
        wait_all(load_x.at[it], load_send.at[it])
        wait_all(load_y.at[it], load_send.at[ITERS + it])
    reduction_ref[...] = finish_sum(SUMS - 1) / start_energy
    for k in range(SUMS):
        wait_all(sums_in.at[k], sum_send.at[k])


def local(nx, ny, rhs, stiff_inverse, schur, phi, coarse_inverse, incidence, pairing):
    n = nx * ny
    faces, cases = rhs.shape[4], rhs.shape[5]
    interface = stiff_inverse.shape[3]
    corners = phi.shape[3]
    coarse_rows, coarse = coarse_inverse.shape
    nodes = incidence.shape[3]
    group = min(GROUP, ny)
    wide = max(window(f, faces)[2] for f in range(4))
    vmem = pl.BlockSpec(memory_space=pltpu.VMEM)
    anywhere = pl.BlockSpec(memory_space=pl.ANY)
    dma = pltpu.SemaphoreType.DMA
    multipliers, reduction = pl.pallas_call(
        functools.partial(kernel, nx, ny),
        out_shape=(
            jax.ShapeDtypeStruct((3, faces, cases), F32),
            jax.ShapeDtypeStruct((1, cases), F32),
        ),
        in_specs=[anywhere] * 3 + [vmem] * 4,
        out_specs=(vmem, vmem),
        scratch_shapes=[
            pltpu.VMEM((3, faces, cases), F32),
            pltpu.VMEM((interface, interface), BF16),
            pltpu.VMEM((interface, interface), BF16),
            pltpu.VMEM((corners, interface), F32),
            pltpu.VMEM((corners, interface), BF16),
            pltpu.VMEM((interface, corners), BF16),
            pltpu.VMEM((4, faces, corners), BF16),
            pltpu.VMEM((4, corners, wide), F32),
            pltpu.VMEM((2, faces, cases), F32),
            pltpu.VMEM((2, 3, faces), jnp.int32),
            pltpu.VMEM((EXCHANGES, 4, faces, cases), F32),
            pltpu.VMEM((interface, cases), F32),
            pltpu.VMEM((ITERS, interface, cases), F32),
            pltpu.VMEM((EXCHANGES, interface, cases), F32),
            pltpu.VMEM((SUMS, 1, cases), F32),
            pltpu.VMEM((SUMS, n, 1, cases), F32),
            pltpu.VMEM((nodes, 128), F32),
            pltpu.VMEM((ny, nx, nodes, 128), F32),
            pltpu.VMEM((ny, nx, coarse_rows, coarse), F32),
            pltpu.VMEM((coarse, coarse), F32),
            pltpu.VMEM((5 * corners, coarse), F32),
            pltpu.VMEM((coarse, group * nx * corners // 2), BF16),
            pltpu.VMEM((ITERS, nx, corners, cases), F32),
            pltpu.VMEM((ITERS, ny, nx * corners // 2, cases), F32),
            dma((3,)),
            dma((8,)),
            dma((8,)),
            dma((EXCHANGES, 4)),
            dma((EXCHANGES, 4)),
            dma((SUMS,)),
            dma((SUMS,)),
            dma((4,)),
            dma((4,)),
            dma((2 * ITERS,)),
            dma((2 * ITERS,)),
        ],
        compiler_params=pltpu.CompilerParams(
            collective_id=0, has_side_effects=True, vmem_limit_bytes=67043328
        ),
    )(
        rhs.reshape(3, faces, cases),
        stiff_inverse.reshape(interface, interface),
        schur.reshape(interface, interface),
        phi.reshape(corners, interface),
        coarse_inverse,
        incidence.reshape(1, nodes),
        pairing.reshape(3, faces),
    )
    return multipliers.reshape(rhs.shape), reduction.reshape(cases)


def solution(mesh):
    nx, ny = mesh.shape["gx"], mesh.shape["gy"]
    return jax.shard_map(
        functools.partial(local, nx, ny),
        mesh=mesh,
        in_specs=(
            P("gx", "gy", None, None, None, None),
            P("gx", "gy", None, None, None),
            P("gx", "gy", None, None, None),
            P("gx", "gy", None, None, None),
            P(("gx", "gy"), None),
            P("gx", "gy", None, None),
            P("gx", "gy", None, None, None),
        ),
        out_specs=(P("gx", "gy", None, None, None, None), P()),
        check_vma=False,
    )
```
